768 devices in a mesh: lat: 12 (over z), rad: 64 (over x, y, core).
Axes of the slice: x: 4, y: 8, z: 12, core: 2. Of those that a mesh axis runs over, the one named last changes fastest.
Arguments:
- positions: float32 [98304, 3, 128], P(('lat', 'rad')), may hold values from 0 to 1
- fields: bfloat16 [98304, 16, 128], P(('lat', 'rad')), may hold values from -6 to 6
- velocity: float32 [81, 196608], P(None, ('lat', 'rad')), may hold values from -3 to 3
- counts: int32 [768], P(('lat', 'rad')), may hold values from 1 to 128, as said below
- elements: int32 [3, 98304], P(None, ('lat', 'rad')), may hold values from 0 to 255
- routes: int32 [2, 98304], P(None, ('lat', 'rad')), may hold values from 0 to 191, as said below
Outputs:
- moved: float32 [147456, 3, 128], P(('lat', 'rad'))
- projected: float32 [27, 16, 196608], P(None, None, ('lat', 'rad'))
The draws below stay inside these ranges and needn't reach their ends.
Inputs may be any that keep to these rules, and one draw needn't show every extreme that they name: counts[d] is at most 128 and equals 128 on some device. Both rows code destinations as in the reference program. routes[0] differs between any two blocks of one device; routes[1] differs between any two blocks that routes[0] sends to the same device.
All inputs are finite; a program needn't handle non-finite values.
Results may differ from the reference program's by a relative error of at most 0.0003.
Values sent between devices are 32-bit elements; how exact they have to be, the bound alone decides.
A program may use at most 32 MiB of HBM per device.

```python
import jax
import jax.numpy as jnp
from jax import lax

BLOCK = 128
FIELDS = 16
MB = 128
NE = 256
CAP = 1
SLOTS = 192
BLOCKS = 98304
ELEMS = 196608
N_LAT = 12
N_RAD = 64
DEVICES = 768


def draw_counts(key, part):
    keys = jax.random.split(jax.random.fold_in(key, 11), 2)
    lowest = max(1, MB // 4)
    drawn = jax.random.randint(keys[0], (DEVICES,), lowest, MB + 1)
    fullest = jax.random.randint(keys[1], (), 0, DEVICES)
    return jnp.where(jnp.arange(DEVICES) == fullest, MB, drawn).astype(jnp.int32)


def shuffled(key, height, width):
    scores = jax.random.randint(key, (height, width), 0, 1 << 20) * width + jnp.arange(width)[None, :]
    return jnp.argsort(scores, axis=1).astype(jnp.int32)


def draw_routes(key, part):
    keys = jax.random.split(jax.random.fold_in(key, 23), 2)
    first_route = shuffled(keys[0], DEVICES, SLOTS)[:, :MB].reshape(-1)
    home = jnp.arange(DEVICES * MB, dtype=jnp.int32) // MB
    lat_step = first_route // (N_RAD * CAP)
    mid_rad = first_route // CAP % N_RAD
    mid_place = first_route % CAP
    middle = (home // N_RAD + lat_step - 1) % N_LAT * N_RAD + mid_rad
    arrival = (lat_step * N_RAD + home % N_RAD) * CAP + mid_place
    second_route = shuffled(keys[1], DEVICES, SLOTS)[middle, arrival]
    return jnp.stack([first_route, second_route]).astype(jnp.int32)


def set_ends(result, key, smallest, top_value):
    place = [jax.random.randint(jax.random.fold_in(key, axis), (), 0, length) for axis, length in enumerate(result.shape)]
    longest = result.shape.index(max(result.shape))
    next_to = place[:longest] + [(place[longest] + 1) % result.shape[longest]] + place[longest + 1:]
    return result.at[tuple(place)].set(smallest).at[tuple(next_to)].set(top_value)


def block_levels(key, shape, cuts, least, top_value):
    loudness = 1.0
    for position, blocks in cuts:
        steps = jax.random.uniform(jax.random.fold_in(jax.random.fold_in(key, 6), position), (blocks,), jnp.float32, least / len(cuts), top_value / len(cuts))
        loudness = loudness * jnp.repeat(jnp.exp(steps), shape[position] // blocks).reshape((-1,) + (1,) * (len(shape) - 1 - position))
    return loudness


def bell_draw(rng, dims, deviation, limit, pieces=(), kind=jnp.bfloat16):
    result = deviation * jax.random.normal(rng, dims, jnp.float32)
    if pieces:
        result = result * block_levels(rng, dims, pieces, -0.22, 0.18)
    return jnp.clip(result, -limit, limit).astype(kind)


def setup_inputs(seed: int = 0) -> dict:
    seeds = jax.random.split(jax.random.key(seed), 7)
    return {
        "positions": jnp.clip(1.0 * jax.random.uniform(seeds[0], (BLOCKS, 3, BLOCK), jnp.float32) ** block_levels(seeds[0], (BLOCKS, 3, BLOCK), ((0, 768),), -0.2, 0.2), 0.0, 1.0),
        "fields": bell_draw(seeds[1], (BLOCKS, FIELDS, BLOCK), 1.0, 6.0, ((0, 768),)),
        "velocity": bell_draw(seeds[2], (81, ELEMS), 0.5, 3.0, ((1, 768),), jnp.float32),
        "counts": draw_counts(jax.random.fold_in(seeds[6], 71), 0),
        "elements": set_ends(jax.random.randint(seeds[4], (3, BLOCKS), 0, NE), jax.random.fold_in(seeds[4], 1), 0, NE - 1).astype(jnp.int32),
        "routes": draw_routes(jax.random.fold_in(seeds[6], 71), 0),
    }


time_step = 0.4
exact = lax.Precision.HIGHEST


def lagrange(coord):
    first_node = 2.0 * (coord - 0.5) * (coord - 1.0)
    middle_node = -4.0 * coord * (coord - 1.0)
    last_node = 2.0 * coord * (coord - 0.5)
    return jnp.stack([first_node, middle_node, last_node], axis=0)


def basis(points):
    along_x = lagrange(points[:, 0, :])
    along_y = lagrange(points[:, 1, :])
    along_z = lagrange(points[:, 2, :])
    table = along_x[:, None, None] * along_y[None, :, None] * along_z[None, None, :]
    return jnp.moveaxis(table.reshape(27, points.shape[0], points.shape[2]), 0, 1)


def speed(columns, points):
    coefficients = columns.T.reshape(points.shape[0], 3, 27)
    return jnp.einsum("scn,snb->scb", coefficients, basis(points), precision=exact)


def reference(positions, fields, velocity, counts, elements, routes):
    devices = N_LAT * N_RAD
    total = positions.shape[0]
    width = positions.shape[2]
    order = jnp.arange(total, dtype=jnp.int32)
    home = order // MB
    valid = (order % MB) < counts[home]
    lat_step = routes[0] // (N_RAD * CAP)
    mid_rad = (routes[0] // CAP) % N_RAD
    mid_lat = (home // N_RAD + lat_step - 1) % N_LAT
    middle = mid_lat * N_RAD + mid_rad
    next_step = routes[1] // (N_RAD * CAP)
    final_rad = (routes[1] // CAP) % N_RAD
    final_place = routes[1] % CAP
    final = ((mid_lat + next_step - 1) % N_LAT) * N_RAD + final_rad
    out_rows = (final * SLOTS + (next_step * N_RAD + mid_rad) * CAP + final_place).astype(jnp.int32)
    start_cols = (home * NE + elements[0]).astype(jnp.int32)
    middle_cols = (middle * NE + elements[1]).astype(jnp.int32)
    final_cols = (final * NE + elements[2]).astype(jnp.int32)

    def advance(block_set):
        points, fractions, start, middle_col = block_set
        first_speed = speed(jnp.take(velocity, start, axis=1), points)
        midway = points + (0.5 * time_step) * first_speed
        landed = points + time_step * speed(jnp.take(velocity, middle_col, axis=1), midway)
        shapes = basis(landed)
        moments = jnp.einsum("snb,sfb->snf", shapes, fractions.astype(jnp.float32), precision=exact)
        return landed, moments, jnp.sum(shapes * shapes, axis=2)

    landed, moments, weights = lax.map(advance, (positions.reshape(devices, MB, 3, width), fields.reshape(devices, MB, fields.shape[1], width), start_cols.reshape(devices, MB), middle_cols.reshape(devices, MB)))
    landed = landed.reshape(total, 3, width)
    moments = moments.reshape(total, 27, fields.shape[1])
    weights = weights.reshape(total, 27)
    live = valid.astype(jnp.float32)
    moved = jnp.zeros((devices * SLOTS, 3, width), jnp.float32).at[out_rows].set(landed * live[:, None, None])
    totals = jax.ops.segment_sum(moments * live[:, None, None], final_cols, num_segments=devices * NE)
    summed = jax.ops.segment_sum(weights * live[:, None], final_cols, num_segments=devices * NE)
    projected = totals / (1.0 + summed[:, :, None])
    return moved, jnp.transpose(projected, (1, 2, 0))
```

```python
import functools

import jax
import jax.numpy as jnp
from jax import lax
from jax.experimental import pallas as pl
from jax.experimental.pallas import tpu as pltpu
from jax.sharding import PartitionSpec as P

time_step = 0.4
exact = lax.Precision.HIGHEST
MESH = pl.DeviceIdType.MESH
LANES = 128
NX, NY, NC = 4, 8, 2


def lagrange(coord):
    first_node = 2.0 * (coord - 0.5) * (coord - 1.0)
    middle_node = -4.0 * coord * (coord - 1.0)
    last_node = 2.0 * coord * (coord - 0.5)
    return jnp.stack([first_node, middle_node, last_node], axis=0)


def basis(points):
    along_x = lagrange(points[:, 0, :])
    along_y = lagrange(points[:, 1, :])
    along_z = lagrange(points[:, 2, :])
    table = along_x[:, None, None] * along_y[None, :, None] * along_z[None, None, :]
    return jnp.moveaxis(table.reshape(27, points.shape[0], points.shape[2]), 0, 1)


def speed(coefficients, points):
    return jnp.einsum("scn,snb->scb", coefficients.reshape(-1, 3, 27), basis(points), precision=exact)


def exchange_kernel(lat_count, rad_count, rows, back, x_ref, o_ref, lsem, ssem, rsem):
    lat = lax.axis_index("lat")
    rad = lax.axis_index("rad")
    places = 3 * rad_count
    x0, y0, c0 = rad // (NY * NC), lax.rem(rad // NC, NY), lax.rem(rad, NC)

    def partner(i):
        m = NY - 1 - lax.rem(i, NY)
        h = (m + 1) // 2
        dy = lax.rem(jnp.where(lax.rem(m, 2) == 1, h, NY - h), NY)
        j = i // NY
        dc = lax.rem(j, NC)
        dx = lax.rem(j // NC + lax.rem(m, NX), NX)
        return (lax.rem(x0 + dx, NX) * NY + lax.rem(y0 + dy, NY)) * NC + lax.rem(c0 + dc, NC)

    def over_partners(act):
        def step(i, carry):
            q = partner(i)
            for k in range(3):
                shift = (1 - k) if back else (k - 1)
                target = (lax.rem(lat + shift + lat_count, lat_count), q)
                if k == 1:
                    @pl.when(q != rad)
                    def _():
                        act(k, q, target)
                else:
                    act(k, q, target)
            return carry

        lax.fori_loop(0, rad_count, step, 0)

    barrier = pltpu.get_barrier_semaphore()
    over_partners(
        lambda k, q, target: pl.semaphore_signal(barrier, inc=1, device_id=target, device_id_type=MESH)
    )
    pl.semaphore_wait(barrier, places - 1)

    def send(k, q, target):
        pltpu.make_async_remote_copy(
            src_ref=x_ref.at[k * rad_count + q, pl.ds(0, rows)],
            dst_ref=o_ref.at[k * rad_count + rad, pl.ds(0, rows)],
            send_sem=ssem, recv_sem=rsem, device_id=target, device_id_type=MESH,
        ).start()

    over_partners(send)
    mine = rad_count + rad
    local = pltpu.make_async_copy(x_ref.at[mine, pl.ds(0, rows)], o_ref.at[mine, pl.ds(0, rows)], lsem)
    local.start()
    local.wait()
    span = o_ref.at[pl.ds(0, places - 1), pl.ds(0, rows)]
    pltpu.make_async_copy(span, span, rsem).wait()
    pltpu.make_async_copy(span, span, ssem).wait()


def exchange(x, rows, back, number):
    lat_count, rad_count = lax.axis_size("lat"), lax.axis_size("rad")
    return pl.pallas_call(
        functools.partial(exchange_kernel, lat_count, rad_count, rows, back),
        out_shape=jax.ShapeDtypeStruct(x.shape, x.dtype),
        in_specs=[pl.BlockSpec(memory_space=pltpu.VMEM)],
        out_specs=pl.BlockSpec(memory_space=pltpu.VMEM),
        scratch_shapes=[pltpu.SemaphoreType.DMA, pltpu.SemaphoreType.DMA, pltpu.SemaphoreType.DMA],
        compiler_params=pltpu.CompilerParams(collective_id=number, has_side_effects=True),
        name=f"exchange{number}",
    )(x)


def place_rows(target, valid, number):
    matches = (target[:, None] == jnp.arange(number, dtype=jnp.int32)[None, :]) & valid[:, None]
    present = jnp.any(matches, axis=0)
    source = jnp.sum(jnp.where(matches, jnp.arange(target.shape[0], dtype=jnp.int32)[:, None], 0), axis=0)
    return source, present


def arrange(member, source, present):
    picked = jnp.take(member, source, axis=0)
    return jnp.where(present.reshape((-1,) + (1,) * (member.ndim - 1)), picked, 0.0)


def widen(flat, rows):
    flat = jnp.pad(flat, ((0, 0), (0, rows * LANES - flat.shape[1])))
    return flat.reshape(-1, rows, LANES)


def per_device(positions, fields, velocity, counts, elements, routes):
    rad_count = lax.axis_size("rad")
    places = 3 * rad_count
    blocks = positions.shape[0]
    owned = velocity.shape[1]
    table = velocity.T
    home_valid = jnp.arange(blocks, dtype=jnp.int32) < counts[0]
    source, present = place_rows(routes[0], home_valid, places)
    labels = jnp.stack(
        [home_valid.astype(jnp.int32), elements[1], routes[1], elements[2]], axis=1
    ).astype(jnp.float32)
    asked = exchange(widen(arrange(labels, source, present), 8), 1, False, 0)[:, 0, :4].astype(jnp.int32)
    first_speed = speed(jnp.take(table, elements[0], axis=0), positions)
    midway = positions + 0.5 * time_step * first_speed
    mid_valid = asked[:, 0] > 0
    answered = exchange(widen(jnp.take(table, asked[:, 1], axis=0), 8), 1, True, 1)[:, 0, :81]
    landed = positions + time_step * speed(jnp.take(answered, routes[0], axis=0), midway)
    shapes = basis(landed)
    moments = jnp.einsum("snb,sfb->snf", shapes, fields.astype(jnp.float32), precision=exact)
    weights = jnp.sum(shapes * shapes, axis=2)
    cargo = jnp.concatenate([landed.reshape(blocks, -1), moments.reshape(blocks, -1), weights], axis=1)
    cargo = exchange(arrange(widen(cargo, 8), source, present), 7, False, 2)
    source, present = place_rows(asked[:, 2], mid_valid, places)
    cargo = cargo.at[:, 6, LANES - 1].set((asked[:, 3] + 1).astype(jnp.float32))
    cargo = exchange(arrange(cargo, source, present), 7, False, 3)
    tags = cargo[:, 6, LANES - 1].astype(jnp.int32) - 1
    cargo = cargo.reshape(places, -1)
    moved = cargo[:, : 3 * LANES].reshape(places, 3, LANES)
    hits = (tags[:, None] == jnp.arange(owned, dtype=jnp.int32)[None, :]).astype(jnp.float32)
    start = 3 * LANES
    totals = jnp.einsum("sm,se->me", cargo[:, start : start + 432], hits, precision=exact)
    summed = jnp.einsum("sn,se->ne", cargo[:, start + 432 : start + 459], hits, precision=exact)
    projected = totals.reshape(27, 16, owned) / (1.0 + summed[:, None, :])
    return moved, projected


def solution(mesh):
    in_specs = (
        P(("lat", "rad"), None, None),
        P(("lat", "rad"), None, None),
        P(None, ("lat", "rad")),
        P(("lat", "rad")),
        P(None, ("lat", "rad")),
        P(None, ("lat", "rad")),
    )
    out_specs = (P(("lat", "rad"), None, None), P(None, None, ("lat", "rad")))
    return jax.shard_map(
        per_device, mesh=mesh, in_specs=in_specs, out_specs=out_specs, check_vma=False
    )
```

```python
import functools

import jax
import jax.numpy as jnp
from jax import lax
from jax.experimental import pallas as pl
from jax.experimental.pallas import tpu as pltpu
from jax.sharding import PartitionSpec as P

time_step = 0.4
exact = lax.Precision.HIGHEST
MESH = pl.DeviceIdType.MESH
LANES = 128
GROUP = 8
NX, NY, NC = 4, 8, 2
NODES = 27
COLUMNS = 3 * NODES
ASKED, ROUTE, HOME = 81, 82, 83
WEIGHTS, TAG = 48, 127
CHUNKS = ((3, 0), (1, 2))
NT = (((1,), (1,)), ((), ()))
TN = (((0,), (0,)), ((), ()))


def product(a, b, dims=(((1,), (0,)), ((), ()))):
    return lax.dot_general(a, b, dims, precision=exact, preferred_element_type=jnp.float32)


def iota(shape, axis):
    return lax.broadcasted_iota(jnp.int32, shape, axis)


def onehot(mask):
    return jnp.where(mask, 1.0, 0.0)


def lagrange(s):
    return 2.0 * (s - 0.5) * (s - 1.0), -4.0 * s * (s - 1.0), 2.0 * s * (s - 0.5)


def speed(coefficients, points):
    along = [lagrange(p) for p in points]
    result = []
    for c in range(3):
        total = None
        for i in range(3):
            plane = None
            for j in range(3):
                line = None
                for k in range(3):
                    n = c * NODES + 9 * i + 3 * j + k
                    term = coefficients[:, n : n + 1] * along[2][k]
                    line = term if line is None else line + term
                line = line * along[1][j]
                plane = line if plane is None else plane + line
            plane = plane * along[0][i]
            total = plane if total is None else total + plane
        result.append(total)
    return result


def basis(points):
    along = [lagrange(p) for p in points]
    shapes = []
    for i in range(3):
        for j in range(3):
            both = along[0][i] * along[1][j]
            for k in range(3):
                shapes.append(both * along[2][k])
    return shapes


def halves(x):
    high = x.astype(jnp.bfloat16)
    return jnp.concatenate([high, (x - high.astype(jnp.float32)).astype(jnp.bfloat16)], axis=0)


def kernel(
    lat_count, rad_count, blocks, owned,
    counts, elements, routes, positions, fields, velocity,
    moved, totals,
    raw, pos, fld, vel, grid, coef, mid, mom, lnd,
    req_s, req_r, rep_s, rep_r, pos_s, pos_r, lnd_s, one_s, one_r, two_s, two_r,
    load_sems, self_sem, send_sems, recv_sems,
):
    lat = lax.axis_index("lat")
    rad = lax.axis_index("rad")
    places = 3 * rad_count
    mine = rad_count + rad
    x0, y0, c0 = rad // (NY * NC), lax.rem(rad // NC, NY), lax.rem(rad, NC)

    def lat_at(shift):
        return lax.rem(lat + shift + lat_count, lat_count)

    def over_partners(act, back=False):
        lats = [lat_at((1 - k) if back else (k - 1)) for k in range(3)]

        def step(j, carry):
            for m in reversed(range(NY)):
                dy = ((m + 1) // 2 if m % 2 else NY - (m + 1) // 2) % NY
                x = lax.rem(x0 + j // NC + m % NX, NX)
                y = lax.rem(y0 + dy, NY)
                q = (x * NY + y) * NC + lax.rem(c0 + j, NC)
                for k in range(3):
                    if k == 1 and m == 0:
                        @pl.when(j != 0)
                        def _():
                            act(k, q, (lats[k], q))
                    else:
                        act(k, q, (lats[k], q))
            return carry

        lax.fori_loop(0, NX * NC, step, 0)

    def send(source, target, number, rows, back=False):
        local = pltpu.make_async_copy(
            source.at[mine, pl.ds(0, rows)], target.at[mine, pl.ds(0, rows)], self_sem
        )
        local.start()

        def act(k, q, device):
            pltpu.make_async_remote_copy(
                src_ref=source.at[k * rad_count + q, pl.ds(0, rows)],
                dst_ref=target.at[k * rad_count + rad, pl.ds(0, rows)],
                send_sem=send_sems.at[number], recv_sem=recv_sems.at[number],
                device_id=device, device_id_type=MESH,
            ).start()

        over_partners(act, back)
        local.wait()

    def settle(buffer, sems, number, rows):
        span = buffer.at[pl.ds(0, places - 1), pl.ds(0, rows)]
        pltpu.make_async_copy(span, span, sems.at[number]).wait()

    loads = [
        pltpu.make_async_copy(velocity, raw, load_sems.at[0]),
        pltpu.make_async_copy(positions, pos, load_sems.at[1]),
        pltpu.make_async_copy(fields, fld, load_sems.at[2]),
    ]
    for load in loads:
        load.start()
    barrier = pltpu.get_barrier_semaphore()
    over_partners(
        lambda k, q, device: pl.semaphore_signal(barrier, inc=1, device_id=device, device_id_type=MESH)
    )

    live = iota((1, blocks), 1) < counts[0]
    element = elements[...]
    route = routes[...]
    first_route = jnp.where(live, route[0:1], -1)
    to_place = onehot(iota((places, blocks), 0) == first_route)
    loads[0].wait()
    vel[pl.ds(80, 48), :] = jnp.zeros((48, owned), jnp.float32)
    vel[pl.ds(0, COLUMNS), :] = raw[...]
    start_hits = onehot(iota((owned, blocks), 0) == element[0:1])
    row = iota((LANES, blocks), 0)
    labels = jnp.where(
        row == ASKED, element[1:2] + 1, jnp.where(row == ROUTE, route[1:2], jnp.where(row == HOME, first_route, 0))
    )
    columns = product(vel[...], start_hits) + labels.astype(jnp.float32)
    req_s[:, 0, :] = product(to_place, columns, NT)
    pl.semaphore_wait(barrier, places - 1)
    send(req_s, req_r, 0, 1)

    grid[...] = columns.T
    loads[1].wait()
    for c in range(3):
        pos_s[:, c, :] = product(to_place, pos[:, c, :])

    def first_step(g, carry):
        rows = pl.ds(pl.multiple_of(g * GROUP, GROUP), GROUP)
        points = [pos[rows, c, :] for c in range(3)]
        for c, u in enumerate(speed(grid[rows, :], points)):
            mid[c, rows, :] = points[c] + 0.5 * time_step * u
        return carry

    lax.fori_loop(0, blocks // GROUP, first_step, 0)

    settle(req_r, recv_sems, 0, 1)
    asked = req_r[:, 0, :]
    middle_hits = onehot(iota((places, owned), 1) == asked[:, ASKED : ASKED + 1].astype(jnp.int32) - 1)
    rep_s[:, 0, :] = product(middle_hits, vel[...], NT)
    send(rep_s, rep_r, 1, 1, back=True)
    send(pos_s, pos_r, 2, 3)
    pick = onehot(iota((GROUP, LANES), 1) == iota((GROUP, LANES), 0) + ASKED)
    turned = product(pick, asked, NT)
    second_route = jnp.where(turned[0:1] > 0.5, turned[1:2].astype(jnp.int32), -1)
    to_final = onehot(iota((places, places), 0) == second_route)
    loads[2].wait()

    settle(rep_r, recv_sems, 1, 1)
    from_place = onehot(iota((blocks, places), 1) == grid[:, HOME : HOME + 1].astype(jnp.int32))
    coef[...] = product(from_place, rep_r[:, 0, :])
    lane = iota((GROUP, LANES), 1)
    own = lane // 16 == iota((GROUP, LANES), 0)
    every = jnp.ones((LANES, LANES), jnp.bfloat16)

    def second_step(g, carry):
        rows = pl.ds(pl.multiple_of(g * GROUP, GROUP), GROUP)
        points = [mid[c, rows, :] for c in range(3)]
        moves = speed(coef[rows, :], points)
        shapes = jnp.concatenate(basis([pos[rows, c, :] + time_step * moves[c] for c in range(3)]), axis=0)
        count = NODES * GROUP
        block_fields = fld[rows].reshape(GROUP * 16, LANES)
        crossed = lax.dot_general(halves(shapes), block_fields, NT, preferred_element_type=jnp.float32)
        crossed = crossed[:count] + crossed[count:]
        squares = lax.dot_general(
            halves(shapes * shapes), every, NT, preferred_element_type=jnp.float32
        )
        squares = squares[:count] + squares[count:]
        for r in range(4):
            total = jnp.zeros((GROUP, LANES), jnp.float32)
            for n in range(8 * r, min(8 * r + 8, NODES)):
                part = jnp.where(own, crossed[n * GROUP : (n + 1) * GROUP], 0.0)
                total += pltpu.roll(part, 16 * (n - 8 * r), 1) if n % 8 else part
            for bit in range(3):
                shift = 16 << bit
                odd = (iota((GROUP, LANES), 0) // (1 << bit)) % 2 == 1
                total = jnp.where(odd, pltpu.roll(total, LANES - shift, 1), total)
            if r == 3:
                for n in range(NODES):
                    total = jnp.where(lane == WEIGHTS + n, squares[n * GROUP : (n + 1) * GROUP], total)
            mom[r, rows, :] = total
        return carry

    lax.fori_loop(0, blocks // GROUP, second_step, 0)
    tags = product(
        onehot(iota((LANES, blocks), 0) == iota((LANES, blocks), 1)),
        jnp.where(iota((LANES, blocks), 0) == TAG, element[2:3] + 1, 0).astype(jnp.float32), NT,
    )
    mom[3] = mom[3] + jnp.where(iota((blocks, LANES), 1) == TAG, tags, 0.0)
    for number, chunk in enumerate(CHUNKS):
        for place, r in enumerate(chunk):
            one_s[number, :, place, :] = product(to_place, mom[r])
        send(one_s.at[number], one_r.at[number], 3 + number, len(chunk))

    settle(pos_r, recv_sems, 2, 3)

    def middle_step(g, carry):
        rows = pl.ds(pl.multiple_of(g * GROUP, GROUP), GROUP)
        points = [pos_r[rows, c, :] for c in range(3)]
        first = speed(req_r[rows, 0, :], points)
        halfway = [points[c] + 0.5 * time_step * first[c] for c in range(3)]
        second = speed(rep_s[rows, 0, :], halfway)
        for c in range(3):
            lnd[c, rows, :] = points[c] + time_step * second[c]
        return carry

    lax.fori_loop(0, places // GROUP, middle_step, 0)
    for c in range(3):
        lnd_s[:, c, :] = product(to_final, lnd[c])
    send(lnd_s, moved, 7, 3)

    for number, chunk in enumerate(CHUNKS):
        settle(one_r.at[number], recv_sems, 3 + number, len(chunk))
        for place in range(len(chunk)):
            two_s[number, :, place, :] = product(to_final, one_r[number, :, place, :])
        send(two_s.at[number], two_r.at[number], 5 + number, len(chunk))

    hits = None
    for number, chunk in enumerate(CHUNKS):
        settle(two_r.at[number], recv_sems, 5 + number, len(chunk))
        for place, r in enumerate(chunk):
            arrived = two_r[number, :, place, :]
            if hits is None:
                hits = onehot(iota((places, owned), 1) == arrived[:, TAG : TAG + 1].astype(jnp.int32) - 1)
            totals[pl.ds(r * LANES, LANES), :] = product(arrived, hits, TN)
    settle(moved, recv_sems, 7, 3)
    for number, (buffer, rows) in enumerate(
        [(req_r, 1), (rep_r, 1), (pos_r, 3), (one_r.at[0], 2), (one_r.at[1], 2), (two_r.at[0], 2), (two_r.at[1], 2), (moved, 3)]
    ):
        settle(buffer, send_sems, number, rows)


def per_device(positions, fields, velocity, counts, elements, routes):
    lat_count, rad_count = lax.axis_size("lat"), lax.axis_size("rad")
    places = 3 * rad_count
    blocks = positions.shape[0]
    owned = velocity.shape[1]
    buffer = pltpu.VMEM((places, 8, LANES), jnp.float32)
    pair = pltpu.VMEM((2, places, 8, LANES), jnp.float32)
    vmem = pl.BlockSpec(memory_space=pltpu.VMEM)
    anywhere = pl.BlockSpec(memory_space=pl.ANY)
    moved, totals = pl.pallas_call(
        functools.partial(kernel, lat_count, rad_count, blocks, owned),
        out_shape=[
            jax.ShapeDtypeStruct((places, 8, LANES), jnp.float32),
            jax.ShapeDtypeStruct((4 * LANES, owned), jnp.float32),
        ],
        in_specs=[pl.BlockSpec(memory_space=pltpu.SMEM), vmem, vmem, anywhere, anywhere, anywhere],
        out_specs=[vmem, vmem],
        scratch_shapes=[
            pltpu.VMEM(velocity.shape, jnp.float32),
            pltpu.VMEM(positions.shape, jnp.float32),
            pltpu.VMEM(fields.shape, fields.dtype),
            pltpu.VMEM((LANES, owned), jnp.float32),
            pltpu.VMEM((blocks, LANES), jnp.float32),
            pltpu.VMEM((blocks, LANES), jnp.float32),
            pltpu.VMEM((3, blocks, LANES), jnp.float32),
            pltpu.VMEM((4, blocks, LANES), jnp.float32),
            pltpu.VMEM((3, places, LANES), jnp.float32),
            buffer, buffer, buffer, buffer, buffer, buffer, buffer, pair, pair, pair, pair,
            pltpu.SemaphoreType.DMA((3,)),
            pltpu.SemaphoreType.DMA,
            pltpu.SemaphoreType.DMA((8,)),
            pltpu.SemaphoreType.DMA((8,)),
        ],
        compiler_params=pltpu.CompilerParams(collective_id=0, has_side_effects=True),
        name="advect",
    )(counts, elements, routes, positions, fields, velocity)
    weights = totals[3 * LANES + WEIGHTS : 3 * LANES + WEIGHTS + NODES]
    projected = totals[: NODES * 16].reshape(NODES, 16, owned) / (1.0 + weights[:, None, :])
    return moved[:, :3], projected


def solution(mesh):
    in_specs = (
        P(("lat", "rad"), None, None),
        P(("lat", "rad"), None, None),
        P(None, ("lat", "rad")),
        P(("lat", "rad")),
        P(None, ("lat", "rad")),
        P(None, ("lat", "rad")),
    )
    out_specs = (P(("lat", "rad"), None, None), P(None, None, ("lat", "rad")))
    return jax.shard_map(
        per_device, mesh=mesh, in_specs=in_specs, out_specs=out_specs, check_vma=False
    )
```

```python
import functools

import jax
import jax.numpy as jnp
from jax import lax
from jax.experimental import pallas as pl
from jax.experimental.pallas import tpu as pltpu
from jax.sharding import PartitionSpec as P

time_step = 0.4
MESH = pl.DeviceIdType.MESH
LANES = 128
GROUP = 8
NX, NY, NC = 4, 8, 2
NODES = 27
COLUMNS = 3 * NODES
ASKED, ROUTE = 81, 82
WEIGHTS, TAG = 48, 127
CHUNKS = ((3, 0), (1, 2))
NT = (((1,), (1,)), ((), ()))


def product(a, b, dims=(((1,), (0,)), ((), ()))):
    return lax.dot_general(a, b, dims, preferred_element_type=jnp.float32)


def halves(x, axis):
    high = x.astype(jnp.bfloat16)
    return jnp.concatenate([high, (x - high.astype(jnp.float32)).astype(jnp.bfloat16)], axis=axis)


def iota(shape, axis):
    return lax.broadcasted_iota(jnp.int32, shape, axis)


def onehot(mask):
    return jnp.where(mask, 1.0, 0.0).astype(jnp.bfloat16)


def lagrange(s):
    return 2.0 * (s - 0.5) * (s - 1.0), -4.0 * s * (s - 1.0), 2.0 * s * (s - 0.5)


def speed(coefficient, points):
    along = [lagrange(p) for p in points]
    result = []
    for c in range(3):
        total = None
        for i in range(3):
            plane = None
            for j in range(3):
                line = None
                for k in range(3):
                    term = coefficient(c * NODES + 9 * i + 3 * j + k) * along[2][k]
                    line = term if line is None else line + term
                line = line * along[1][j]
                plane = line if plane is None else plane + line
            plane = plane * along[0][i]
            total = plane if total is None else total + plane
        result.append(total)
    return result


def basis(points):
    along = [lagrange(p) for p in points]
    shapes = []
    for i in range(3):
        for j in range(3):
            both = along[0][i] * along[1][j]
            for k in range(3):
                shapes.append(both * along[2][k])
    return shapes


def kernel(
    lat_count, rad_count, blocks, owned,
    counts, elements, routes, positions, fields, velocity,
    moved, totals,
    raw, pos, fld, vel, posT, midT, lndT, lnd, mom, wts, colT, repT, midcol, midrep, midpos, midlnd,
    req_s, req_r, rep_s, rep_r, pos_s, pos_r, lnd_s, one_s, one_r, two_s, two_r,
    load_sems, self_sem, send_sems, recv_sems,
):
    lat = lax.axis_index("lat")
    rad = lax.axis_index("rad")
    places = 3 * rad_count
    mine = rad_count + rad
    x0, y0, c0 = rad // (NY * NC), lax.rem(rad // NC, NY), lax.rem(rad, NC)

    def lat_at(shift):
        return lax.rem(lat + shift + lat_count, lat_count)

    def over_partners(act, back=False):
        lats = [lat_at((1 - k) if back else (k - 1)) for k in range(3)]

        def step(j, carry):
            for m in reversed(range(NY)):
                dy = ((m + 1) // 2 if m % 2 else NY - (m + 1) // 2) % NY
                x = lax.rem(x0 + j // NC + m % NX, NX)
                y = lax.rem(y0 + dy, NY)
                q = (x * NY + y) * NC + lax.rem(c0 + j, NC)
                for k in range(3):
                    if k == 1 and m == 0:
                        @pl.when(j != 0)
                        def _():
                            act(k, q, (lats[k], q))
                    else:
                        act(k, q, (lats[k], q))
            return carry

        lax.fori_loop(0, NX * NC, step, 0)

    def send(source, target, number, rows, back=False):
        local = pltpu.make_async_copy(
            source.at[mine, pl.ds(0, rows)], target.at[mine, pl.ds(0, rows)], self_sem
        )
        local.start()

        def act(k, q, device):
            pltpu.make_async_remote_copy(
                src_ref=source.at[k * rad_count + q, pl.ds(0, rows)],
                dst_ref=target.at[k * rad_count + rad, pl.ds(0, rows)],
                send_sem=send_sems.at[number], recv_sem=recv_sems.at[number],
                device_id=device, device_id_type=MESH,
            ).start()

        over_partners(act, back)
        local.wait()

    def settle(buffer, sems, number, rows):
        span = buffer.at[pl.ds(0, places - 1), pl.ds(0, rows)]
        pltpu.make_async_copy(span, span, sems.at[number]).wait()

    loads = [
        pltpu.make_async_copy(velocity, raw, load_sems.at[0]),
        pltpu.make_async_copy(positions, pos, load_sems.at[1]),
        pltpu.make_async_copy(fields, fld, load_sems.at[2]),
    ]
    for load in loads:
        load.start()
    barrier = pltpu.get_barrier_semaphore()
    over_partners(
        lambda k, q, device: pl.semaphore_signal(barrier, inc=1, device_id=device, device_id_type=MESH)
    )

    def groups(count, size, act, unroll=1):
        def step(g, carry):
            act(pl.ds(pl.multiple_of(g * size, size), size))
            return carry

        lax.fori_loop(0, count // size, step, 0, unroll=unroll)

    live = iota((1, blocks), 1) < counts[0]
    element = elements[...]
    route = routes[...]
    first_route = jnp.where(live, route[0:1], -1)
    to_place = onehot(iota((places, blocks), 0) == first_route)
    twice = jnp.concatenate([to_place, to_place], axis=1)
    loads[0].wait()
    vel[pl.ds(80, 48), :] = jnp.zeros((48, owned), jnp.float32)
    vel[pl.ds(0, COLUMNS), :] = raw[...]
    columns = halves(vel[...], 0)
    start_hits = onehot(iota((owned, blocks), 0) == element[0:1])
    row = iota((LANES, blocks), 0)
    labels = jnp.where(row == ASKED, element[1:2] + 1, jnp.where(row == ROUTE, route[1:2], 0))
    both = product(columns, start_hits)
    colT[...] = both[:LANES] + both[LANES:] + labels.astype(jnp.float32)
    req_s[:, 0, :] = product(twice, halves(colT[...], 1), NT)
    loads[1].wait()
    for c in range(3):
        pos_s[:, c, :] = product(twice, halves(pos[c], 0))
    pl.semaphore_wait(barrier, places - 1)
    send(req_s, req_r, 0, 1)
    send(pos_s, pos_r, 2, 3)

    for c in range(3):
        posT[c] = pos[c].T

    def first_step(rows):
        points = [posT[c, rows, :] for c in range(3)]
        for c, u in enumerate(speed(lambda n: colT[pl.ds(n, 1), :], points)):
            midT[c, rows, :] = points[c] + 0.5 * time_step * u

    groups(LANES, 16, first_step, 2)

    settle(req_r, recv_sems, 0, 1)
    asked = req_r[:, 0, :]
    middle_hits = onehot(iota((places, owned), 1) == asked[:, ASKED : ASKED + 1].astype(jnp.int32) - 1)
    both = product(middle_hits, columns, NT)
    reply = both[:, :LANES] + both[:, LANES:]
    rep_s[:, 0, :] = reply
    send(rep_s, rep_r, 1, 1, back=True)
    midrep[...] = reply.T
    midcol[...] = asked.T
    second_route = jnp.where(
        midcol[pl.ds(ASKED, 1), :] > 0.5, midcol[pl.ds(ROUTE, 1), :].astype(jnp.int32), -1
    )
    to_final = onehot(iota((places, places), 0) == second_route)
    loads[2].wait()

    settle(pos_r, recv_sems, 2, 3)
    for c in range(3):
        midpos[c] = pos_r[:, c, :].T

    def middle_step(rows):
        points = [midpos[c, rows, :] for c in range(3)]
        first = speed(lambda n: midcol[pl.ds(n, 1), :], points)
        halfway = [points[c] + 0.5 * time_step * first[c] for c in range(3)]
        second = speed(lambda n: midrep[pl.ds(n, 1), :], halfway)
        for c in range(3):
            midlnd[c, rows, :] = points[c] + time_step * second[c]

    groups(LANES, GROUP, middle_step, 2)
    for c in range(3):
        both = product(to_final, halves(midlnd[c], 0), NT)
        lnd_s[:, c, :] = both[:, :LANES] + both[:, LANES:]
    send(lnd_s, moved, 7, 3)

    settle(rep_r, recv_sems, 1, 1)
    both = product(halves(rep_r[:, 0, :].T, 0), to_place)
    repT[...] = both[:LANES] + both[LANES:]

    def second_step(rows):
        points = [midT[c, rows, :] for c in range(3)]
        for c, u in enumerate(speed(lambda n: repT[pl.ds(n, 1), :], points)):
            lndT[c, rows, :] = posT[c, rows, :] + time_step * u

    groups(LANES, 16, second_step, 2)
    for c in range(3):
        lnd[c] = lndT[c].T

    lane = iota((GROUP, LANES), 1)
    own = lane // 16 == iota((GROUP, LANES), 0)
    odd = [(iota((GROUP, LANES), 0) // (1 << bit)) % 2 == 1 for bit in range(3)]

    def moment_step(rows):
        shapes = halves(jnp.concatenate(basis([lnd[c, rows, :] for c in range(3)]), axis=0), 1)
        block_fields = fld[rows].reshape(GROUP * 16, LANES)
        crossed = product(shapes, jnp.concatenate([block_fields, block_fields], axis=1), NT)
        for r in range(4):
            total = None
            for n in range(8 * r, min(8 * r + 8, NODES)):
                part = jnp.where(own, crossed[n * GROUP : (n + 1) * GROUP], 0.0)
                part = pltpu.roll(part, 16 * (n - 8 * r), 1) if n % 8 else part
                total = part if total is None else total + part
            for bit in range(3):
                total = jnp.where(odd[bit], pltpu.roll(total, LANES - (16 << bit), 1), total)
            mom[r, rows, :] = total

    groups(blocks, GROUP, moment_step, 4)

    def weight_step(g, sums):
        rows = pl.ds(pl.multiple_of(g * GROUP, GROUP), GROUP)
        squares = [[v * v for v in lagrange(lndT[c, rows, :])] for c in range(3)]
        result = []
        for i in range(3):
            for j in range(3):
                pair = squares[0][i] * squares[1][j]
                for k in range(3):
                    result.append(sums[len(result)] + pair * squares[2][k])
        return tuple(result)

    sums = lax.fori_loop(
        0, LANES // GROUP, weight_step, tuple(jnp.zeros((GROUP, blocks), jnp.float32) for _ in range(NODES)),
        unroll=2,
    )
    wts[...] = jnp.where(row == TAG, element[2:3] + 1, 0).astype(jnp.float32)
    for n in range(NODES):
        wts[pl.ds(WEIGHTS + n, 1), :] = jnp.sum(sums[n], axis=0, keepdims=True)
    mom[3] = mom[3] + wts[...].T

    for number, chunk in enumerate(CHUNKS):
        placed = product(twice, halves(jnp.concatenate([mom[r] for r in chunk], axis=1), 0))
        for place in range(len(chunk)):
            one_s[number, :, place, :] = placed[:, place * LANES : (place + 1) * LANES]
        send(one_s.at[number], one_r.at[number], 3 + number, len(chunk))

    for number, chunk in enumerate(CHUNKS):
        settle(one_r.at[number], recv_sems, 3 + number, len(chunk))
        wide = len(chunk) * LANES
        arrived = jnp.concatenate([one_r[number, :, place, :] for place in range(len(chunk))], axis=1)
        both = product(to_final, halves(arrived, 1))
        both = both[:, :wide] + both[:, wide:]
        for place in range(len(chunk)):
            two_s[number, :, place, :] = both[:, place * LANES : (place + 1) * LANES]
        send(two_s.at[number], two_r.at[number], 5 + number, len(chunk))

    hits = None
    for number, chunk in enumerate(CHUNKS):
        settle(two_r.at[number], recv_sems, 5 + number, len(chunk))
        if hits is None:
            tag = two_r[number, :, 0, :][:, TAG : TAG + 1].astype(jnp.int32) - 1
            hits = onehot(iota((places, owned), 1) == tag)
        wide = len(chunk) * LANES
        arrived = jnp.concatenate([two_r[number, :, place, :] for place in range(len(chunk))], axis=1)
        both = product(halves(arrived.T, 0), hits)
        both = both[:wide] + both[wide:]
        for place, r in enumerate(chunk):
            totals[pl.ds(r * LANES, LANES), :] = both[place * LANES : (place + 1) * LANES]
    settle(moved, recv_sems, 7, 3)
    for number, (buffer, rows) in enumerate(
        [(req_r, 1), (rep_r, 1), (pos_r, 3), (one_r.at[0], 2), (one_r.at[1], 2), (two_r.at[0], 2), (two_r.at[1], 2), (moved, 3)]
    ):
        settle(buffer, send_sems, number, rows)


def per_device(positions, fields, velocity, counts, elements, routes):
    lat_count, rad_count = lax.axis_size("lat"), lax.axis_size("rad")
    places = 3 * rad_count
    blocks = positions.shape[0]
    owned = velocity.shape[1]
    buffer = pltpu.VMEM((places, 8, LANES), jnp.float32)
    pair = pltpu.VMEM((2, places, 8, LANES), jnp.float32)
    square = pltpu.VMEM((blocks, LANES), jnp.float32)
    square3 = pltpu.VMEM((3, blocks, LANES), jnp.float32)
    vmem = pl.BlockSpec(memory_space=pltpu.VMEM)
    anywhere = pl.BlockSpec(memory_space=pl.ANY)
    moved, totals = pl.pallas_call(
        functools.partial(kernel, lat_count, rad_count, blocks, owned),
        out_shape=[
            jax.ShapeDtypeStruct((places, 8, LANES), jnp.float32),
            jax.ShapeDtypeStruct((4 * LANES, owned), jnp.float32),
        ],
        in_specs=[pl.BlockSpec(memory_space=pltpu.SMEM), vmem, vmem, anywhere, anywhere, anywhere],
        out_specs=[vmem, vmem],
        scratch_shapes=[
            pltpu.VMEM(velocity.shape, jnp.float32),
            square3,
            pltpu.VMEM(fields.shape, fields.dtype),
            pltpu.VMEM((LANES, owned), jnp.float32),
            square3, square3, square3, square3,
            pltpu.VMEM((4, blocks, LANES), jnp.float32),
            square, square, square,
            pltpu.VMEM((LANES, places), jnp.float32),
            pltpu.VMEM((LANES, places), jnp.float32),
            pltpu.VMEM((3, LANES, places), jnp.float32),
            pltpu.VMEM((3, LANES, places), jnp.float32),
            buffer, buffer, buffer, buffer, buffer, buffer, buffer, pair, pair, pair, pair,
            pltpu.SemaphoreType.DMA((3,)),
            pltpu.SemaphoreType.DMA,
            pltpu.SemaphoreType.DMA((8,)),
            pltpu.SemaphoreType.DMA((8,)),
        ],
        compiler_params=pltpu.CompilerParams(collective_id=0, has_side_effects=True),
        name="advect",
    )(counts, elements, routes, jnp.transpose(positions, (1, 0, 2)), fields, velocity)
    weights = totals[3 * LANES + WEIGHTS : 3 * LANES + WEIGHTS + NODES]
    projected = totals[: NODES * 16].reshape(NODES, 16, owned) / (1.0 + weights[:, None, :])
    return moved[:, :3], projected


def solution(mesh):
    in_specs = (
        P(("lat", "rad"), None, None),
        P(("lat", "rad"), None, None),
        P(None, ("lat", "rad")),
        P(("lat", "rad")),
        P(None, ("lat", "rad")),
        P(None, ("lat", "rad")),
    )
    out_specs = (P(("lat", "rad"), None, None), P(None, None, ("lat", "rad")))
    return jax.shard_map(
        per_device, mesh=mesh, in_specs=in_specs, out_specs=out_specs, check_vma=False
    )
```

```python
import functools

import jax
import jax.numpy as jnp
from jax import lax
from jax.experimental import pallas as pl
from jax.experimental.pallas import tpu as pltpu
from jax.sharding import PartitionSpec as P

time_step = 0.4
MESH = pl.DeviceIdType.MESH
LANES = 128
GROUP = 8
NX, NY, NC = 4, 8, 2
NODES = 27
COLUMNS = 3 * NODES
ASKED, ROUTE = 81, 82
WEIGHTS, TAG = 48, 127
CHUNKS = ((0, 1), (2, 3))
NT = (((1,), (1,)), ((), ()))


def product(a, b, dims=(((1,), (0,)), ((), ()))):
    return lax.dot_general(a, b, dims, preferred_element_type=jnp.float32)


def halves(x, axis):
    high = x.astype(jnp.bfloat16)
    return jnp.concatenate([high, (x - high.astype(jnp.float32)).astype(jnp.bfloat16)], axis=axis)


def iota(shape, axis):
    return lax.broadcasted_iota(jnp.int32, shape, axis)


def onehot(mask):
    return jnp.where(mask, 1.0, 0.0).astype(jnp.bfloat16)


def lagrange(s):
    return 2.0 * (s - 0.5) * (s - 1.0), -4.0 * s * (s - 1.0), 2.0 * s * (s - 0.5)


def speed(coefficient, points):
    along = [lagrange(p) for p in points]
    result = []
    for c in range(3):
        total = None
        for i in range(3):
            plane = None
            for j in range(3):
                line = None
                for k in range(3):
                    term = coefficient(c * NODES + 9 * i + 3 * j + k) * along[2][k]
                    line = term if line is None else line + term
                line = line * along[1][j]
                plane = line if plane is None else plane + line
            plane = plane * along[0][i]
            total = plane if total is None else total + plane
        result.append(total)
    return result


def basis(points):
    along = [lagrange(p) for p in points]
    shapes = []
    for i in range(3):
        for j in range(3):
            both = along[0][i] * along[1][j]
            for k in range(3):
                shapes.append(both * along[2][k])
    return shapes


def kernel(
    lat_count, rad_count, blocks, owned,
    counts_hbm, elements_hbm, routes_hbm, positions, fields, velocity,
    placed_out, projected,
    moved, totals, counts, elements, routes,
    raw, pos, fld, vel, posT, midT, lndT, lnd, mom, wts, colT, repT, midcol, midrep, midpos, midlnd,
    req_s, req_r, rep_s, rep_r, pos_s, pos_r, lnd_s, one_s, one_r, two_s, two_r,
    load_sems, self_sem, send_sems, recv_sems,
):
    lat = lax.axis_index("lat")
    rad = lax.axis_index("rad")
    places = 3 * rad_count
    mine = rad_count + rad
    x0, y0, c0 = rad // (NY * NC), lax.rem(rad // NC, NY), lax.rem(rad, NC)

    def lat_at(shift):
        return lax.rem(lat + shift + lat_count, lat_count)

    def over_partners(act, back=False):
        side = 1 - 2 * lax.rem(x0 + y0 + c0, 2)
        lats = [lat_at((1 - k) if back else (k - 1)) for k in range(3)]

        def step(j, carry):
            for m in reversed(range(NY)):
                dy = ((m + 1) // 2 if m % 2 else NY - (m + 1) // 2) % NY
                x = lax.rem(x0 + side * lax.rem(j // NC + m % NX, NX) + NX, NX)
                y = lax.rem(y0 + side * dy + NY, NY)
                q = (x * NY + y) * NC + lax.rem(c0 + j, NC)
                for k in range(3):
                    if k == 1 and m == 0:
                        @pl.when(j != 0)
                        def _():
                            act(k, q, (lats[k], q))
                    else:
                        act(k, q, (lats[k], q))
            return carry

        lax.fori_loop(0, NX * NC, step, 0)

    def send(source, target, number, rows, back=False):
        local = pltpu.make_async_copy(
            source.at[mine, pl.ds(0, rows)], target.at[mine, pl.ds(0, rows)], self_sem
        )
        local.start()

        def act(k, q, device):
            pltpu.make_async_remote_copy(
                src_ref=source.at[k * rad_count + q, pl.ds(0, rows)],
                dst_ref=target.at[k * rad_count + rad, pl.ds(0, rows)],
                send_sem=send_sems.at[number], recv_sem=recv_sems.at[number],
                device_id=device, device_id_type=MESH,
            ).start()

        over_partners(act, back)
        local.wait()

    def settle(buffer, sems, number, rows):
        span = buffer.at[pl.ds(0, places - 1), pl.ds(0, rows)]
        pltpu.make_async_copy(span, span, sems.at[number]).wait()

    barrier = pltpu.get_barrier_semaphore()
    over_partners(
        lambda k, q, device: pl.semaphore_signal(barrier, inc=1, device_id=device, device_id_type=MESH)
    )
    loads = [
        pltpu.make_async_copy(velocity, raw, load_sems.at[0]),
        pltpu.make_async_copy(positions, pos, load_sems.at[1]),
        pltpu.make_async_copy(fields, fld, load_sems.at[2]),
        pltpu.make_async_copy(counts_hbm, counts, load_sems.at[3]),
        pltpu.make_async_copy(elements_hbm, elements, load_sems.at[4]),
        pltpu.make_async_copy(routes_hbm, routes, load_sems.at[5]),
    ]
    for load in loads:
        load.start()
    def groups(count, size, act, unroll=1):
        def step(g, carry):
            act(pl.ds(pl.multiple_of(g * size, size), size))
            return carry

        lax.fori_loop(0, count // size, step, 0, unroll=unroll)

    for load in loads[3:]:
        load.wait()
    live = iota((1, blocks), 1) < counts[0]
    element = elements[...]
    route = routes[...]
    first_route = jnp.where(live, route[0:1], -1)
    to_place = onehot(iota((places, blocks), 0) == first_route)
    twice = jnp.concatenate([to_place, to_place], axis=1)
    loads[0].wait()
    vel[pl.ds(80, 48), :] = jnp.zeros((48, owned), jnp.float32)
    vel[pl.ds(0, COLUMNS), :] = raw[...]
    columns = halves(vel[...], 0)
    start_hits = onehot(iota((owned, blocks), 0) == element[0:1])
    row = iota((LANES, blocks), 0)
    labels = jnp.where(row == ASKED, element[1:2] + 1, jnp.where(row == ROUTE, route[1:2], 0))
    both = product(columns, start_hits)
    colT[...] = both[:LANES] + both[LANES:] + labels.astype(jnp.float32)
    req_s[:, 0, :] = product(twice, halves(colT[...], 1), NT)
    loads[1].wait()
    for c in range(3):
        pos_s[:, c, :] = product(twice, halves(pos[c], 0))
    pl.semaphore_wait(barrier, places - 1)
    send(req_s, req_r, 0, 1)
    send(pos_s, pos_r, 2, 3)

    for c in range(3):
        posT[c] = pos[c].T

    def first_step(rows):
        points = [posT[c, rows, :] for c in range(3)]
        for c, u in enumerate(speed(lambda n: colT[pl.ds(n, 1), :], points)):
            midT[c, rows, :] = points[c] + 0.5 * time_step * u

    groups(LANES, 16, first_step, 2)

    settle(req_r, recv_sems, 0, 1)
    asked = req_r[:, 0, :]
    middle_hits = onehot(iota((places, owned), 1) == asked[:, ASKED : ASKED + 1].astype(jnp.int32) - 1)
    both = product(middle_hits, columns, NT)
    reply = both[:, :LANES] + both[:, LANES:]
    rep_s[:, 0, :] = reply
    send(rep_s, rep_r, 1, 1, back=True)
    midrep[...] = reply.T
    midcol[...] = asked.T
    second_route = jnp.where(
        midcol[pl.ds(ASKED, 1), :] > 0.5, midcol[pl.ds(ROUTE, 1), :].astype(jnp.int32), -1
    )
    to_final = onehot(iota((places, places), 0) == second_route)
    loads[2].wait()

    settle(pos_r, recv_sems, 2, 3)
    for c in range(3):
        midpos[c] = pos_r[:, c, :].T

    def middle_step(rows):
        points = [midpos[c, rows, :] for c in range(3)]
        first = speed(lambda n: midcol[pl.ds(n, 1), :], points)
        halfway = [points[c] + 0.5 * time_step * first[c] for c in range(3)]
        second = speed(lambda n: midrep[pl.ds(n, 1), :], halfway)
        for c in range(3):
            midlnd[c, rows, :] = points[c] + time_step * second[c]

    groups(LANES, GROUP, middle_step, 2)
    for c in range(3):
        both = product(to_final, halves(midlnd[c], 0), NT)
        lnd_s[:, c, :] = both[:, :LANES] + both[:, LANES:]
    send(lnd_s, moved, 7, 3)

    settle(rep_r, recv_sems, 1, 1)
    both = product(halves(rep_r[:, 0, :].T, 0), to_place)
    repT[...] = both[:LANES] + both[LANES:]

    def second_step(rows):
        points = [midT[c, rows, :] for c in range(3)]
        for c, u in enumerate(speed(lambda n: repT[pl.ds(n, 1), :], points)):
            lndT[c, rows, :] = posT[c, rows, :] + time_step * u

    groups(LANES, 16, second_step, 2)
    for c in range(3):
        lnd[c] = lndT[c].T

    lane = iota((GROUP, LANES), 1)
    own = lane // 16 == iota((GROUP, LANES), 0)
    odd = [(iota((GROUP, LANES), 0) // (1 << bit)) % 2 == 1 for bit in range(3)]

    def moment_steps(nodes):
        def moment_step(rows):
            every = basis([lnd[c, rows, :] for c in range(3)])
            shapes = halves(jnp.concatenate([every[n] for n in nodes], axis=0), 1)
            block_fields = fld[rows].reshape(GROUP * 16, LANES)
            crossed = product(shapes, jnp.concatenate([block_fields, block_fields], axis=1), NT)
            lines = {}
            for place, n in enumerate(nodes):
                part = jnp.where(own, crossed[place * GROUP : (place + 1) * GROUP], 0.0)
                part = pltpu.roll(part, 16 * (n % 8), 1) if n % 8 else part
                lines[n // 8] = lines[n // 8] + part if n // 8 in lines else part
            for r, total in lines.items():
                for bit in range(3):
                    total = jnp.where(odd[bit], pltpu.roll(total, LANES - (16 << bit), 1), total)
                mom[r, rows, :] = total

        groups(blocks, GROUP, moment_step, 4)

    def weight_step(g, sums):
        rows = pl.ds(pl.multiple_of(g * GROUP, GROUP), GROUP)
        squares = [[v * v for v in lagrange(lndT[c, rows, :])] for c in range(3)]
        result = []
        for i in range(3):
            for j in range(3):
                pair = squares[0][i] * squares[1][j]
                for k in range(3):
                    result.append(sums[len(result)] + pair * squares[2][k])
        return tuple(result)

    for number, chunk in enumerate(CHUNKS):
        moment_steps([n for n in range(NODES) if n // 8 in chunk])
        if 3 in chunk:
            zeros = tuple(jnp.zeros((GROUP, blocks), jnp.float32) for _ in range(NODES))
            sums = lax.fori_loop(0, LANES // GROUP, weight_step, zeros, unroll=2)
            wts[...] = jnp.where(row == TAG, element[2:3] + 1, 0).astype(jnp.float32)
            for n in range(NODES):
                wts[pl.ds(WEIGHTS + n, 1), :] = jnp.sum(sums[n], axis=0, keepdims=True)
            mom[3] = mom[3] + wts[...].T
        placed = product(twice, halves(jnp.concatenate([mom[r] for r in chunk], axis=1), 0))
        for place in range(len(chunk)):
            one_s[number, :, place, :] = placed[:, place * LANES : (place + 1) * LANES]
        send(one_s.at[number], one_r.at[number], 3 + number, len(chunk))

    for number, chunk in enumerate(CHUNKS):
        settle(one_r.at[number], recv_sems, 3 + number, len(chunk))
        wide = len(chunk) * LANES
        arrived = jnp.concatenate([one_r[number, :, place, :] for place in range(len(chunk))], axis=1)
        both = product(to_final, halves(arrived, 1))
        both = both[:, :wide] + both[:, wide:]
        for place in range(len(chunk)):
            two_s[number, :, place, :] = both[:, place * LANES : (place + 1) * LANES]
        send(two_s.at[number], two_r.at[number], 5 + number, len(chunk))

    settle(moved, recv_sems, 7, 3)
    for c in range(3):
        placed_out[c] = moved[:, c, :]
    turned = []
    for number, chunk in enumerate(CHUNKS):
        settle(two_r.at[number], recv_sems, 5 + number, len(chunk))
        arrived = jnp.concatenate([two_r[number, :, place, :] for place in range(len(chunk))], axis=1)
        turned.append(halves(arrived.T, 0))
    tag = two_r[1, :, CHUNKS[1].index(3), :][:, TAG : TAG + 1].astype(jnp.int32) - 1
    hits = onehot(iota((places, owned), 1) == tag)
    for number, chunk in enumerate(CHUNKS):
        wide = len(chunk) * LANES
        both = product(turned[number], hits)
        both = both[:wide] + both[wide:]
        for place, r in enumerate(chunk):
            totals[pl.ds(r * LANES, LANES), :] = both[place * LANES : (place + 1) * LANES]
    for n in range(NODES):
        weight = totals[pl.ds(3 * LANES + WEIGHTS + n, 1), :]
        projected[pl.ds(16 * n, 16), :] = totals[pl.ds(16 * n, 16), :] / (1.0 + weight)
    for number, (buffer, rows) in enumerate(
        [(req_r, 1), (rep_r, 1), (pos_r, 3), (one_r.at[0], 2), (one_r.at[1], 2), (two_r.at[0], 2), (two_r.at[1], 2), (moved, 3)]
    ):
        settle(buffer, send_sems, number, rows)


def per_device(positions, fields, velocity, counts, elements, routes):
    lat_count, rad_count = lax.axis_size("lat"), lax.axis_size("rad")
    places = 3 * rad_count
    blocks = positions.shape[0]
    owned = velocity.shape[1]
    buffer = pltpu.VMEM((places, 8, LANES), jnp.float32)
    pair = pltpu.VMEM((2, places, 8, LANES), jnp.float32)
    square = pltpu.VMEM((blocks, LANES), jnp.float32)
    square3 = pltpu.VMEM((3, blocks, LANES), jnp.float32)
    vmem = pl.BlockSpec(memory_space=pltpu.VMEM)
    anywhere = pl.BlockSpec(memory_space=pl.ANY)
    placed, projected = pl.pallas_call(
        functools.partial(kernel, lat_count, rad_count, blocks, owned),
        out_shape=[
            jax.ShapeDtypeStruct((3, places, LANES), jnp.float32),
            jax.ShapeDtypeStruct((NODES * 16, owned), jnp.float32),
        ],
        in_specs=[anywhere] * 6,
        out_specs=[vmem, vmem],
        scratch_shapes=[
            buffer,
            pltpu.VMEM((4 * LANES, owned), jnp.float32),
            pltpu.SMEM((1,), jnp.int32),
            pltpu.VMEM(elements.shape, jnp.int32),
            pltpu.VMEM(routes.shape, jnp.int32),
            pltpu.VMEM(velocity.shape, jnp.float32),
            square3,
            pltpu.VMEM(fields.shape, fields.dtype),
            pltpu.VMEM((LANES, owned), jnp.float32),
            square3, square3, square3, square3,
            pltpu.VMEM((4, blocks, LANES), jnp.float32),
            square, square, square,
            pltpu.VMEM((LANES, places), jnp.float32),
            pltpu.VMEM((LANES, places), jnp.float32),
            pltpu.VMEM((3, LANES, places), jnp.float32),
            pltpu.VMEM((3, LANES, places), jnp.float32),
            buffer, buffer, buffer, buffer, buffer, buffer, buffer, pair, pair, pair, pair,
            pltpu.SemaphoreType.DMA((6,)),
            pltpu.SemaphoreType.DMA,
            pltpu.SemaphoreType.DMA((8,)),
            pltpu.SemaphoreType.DMA((8,)),
        ],
        compiler_params=pltpu.CompilerParams(collective_id=0, has_side_effects=True),
        name="advect",
    )(counts, elements, routes, jnp.transpose(positions, (1, 0, 2)), fields, velocity)
    return jnp.transpose(placed, (1, 0, 2)), projected.reshape(NODES, 16, owned)


def solution(mesh):
    in_specs = (
        P(("lat", "rad"), None, None),
        P(("lat", "rad"), None, None),
        P(None, ("lat", "rad")),
        P(("lat", "rad")),
        P(None, ("lat", "rad")),
        P(None, ("lat", "rad")),
    )
    out_specs = (P(("lat", "rad"), None, None), P(None, None, ("lat", "rad")))
    return jax.shard_map(
        per_device, mesh=mesh, in_specs=in_specs, out_specs=out_specs, check_vma=False
    )
```
